32 devices in a mesh: pb: 2 (over y), col: 4 (over z), row: 4 (over x, core).
Axes of the slice: x: 2, y: 2, z: 4, core: 2. Of those that a mesh axis runs over, the one named last changes fastest.
Arguments:
- pair_density: bfloat16 [6144, 6144], P(('pb', 'col'), 'row'), parts along dimension 0, may hold values from -0.19921875 to 0.19921875
- band_pairs: int32 [2, 3072], replicated, may hold values from 0 to 255, as said below
- valence: float32 [256], replicated, may hold values from -12 to -2
- conduction: float32 [12], replicated, may hold values from 1 to 8
- wave_vectors: int32 [3, 12288], P(None, 'pb'), parts along dimension 1, may hold values from -6 to 6
- momentum: float32 [6], P('pb'), parts along dimension 0, may hold values from 0.3 to 0.7
- guess_scale: float32 [12288], P('pb'), parts along dimension 0, may hold values from 0.4 to 0.75
Outputs:
- epsilon: float32 [12288, 6144], P(('pb', 'row'), 'col'), parts along dimension 0
- inverse: float32 [12288, 6144], P(('pb', 'row'), 'col'), parts along dimension 0
The draws below stay inside these ranges and needn't reach their ends.
There are 2 independent parts, one for each index of `pb`. The reference program is written for one: setup_inputs(seed, part) draws one part's arguments, and reference() takes and returns one part's arrays. A program takes and returns all parts, laid end to end along the dimension named above; an argument that names none is the same for every part. Nothing has to cross between parts.
Inputs may be any that keep to these rules, and one draw needn't show every extreme that they name: `band_pairs`: column p names a valence band below 256 in row 0 and a conduction band below 12 in row 1; every such pair of bands appears in exactly one column.
All inputs are finite; a program needn't handle non-finite values.
Results may differ from the reference program's by a relative error of at most 0.0036.
The reference program's roundings to bfloat16 on the way (of `weighted`, `mixed_b` and `square_b`) count: a program that leaves them out, or rounds other values in their place, can miss the bound.
Values may be sent and summed in bfloat16 or wider, within the bound.
A program may use at most 128 MiB of HBM per device.

```python
import math
import jax
import jax.numpy as jnp
from jax import lax

NG = 6144
NV = 256
NC = 12
PAIRS = 3072


def draw_band_pairs(key, part):
    shuffled = jax.random.permutation(jax.random.fold_in(key, 17), NV * NC).astype(jnp.int32)
    return jnp.stack([shuffled // NC, shuffled % NC]).astype(jnp.int32)


def place_ends(result, stream_key, low, high):
    longest = result.shape.index(max(result.shape))
    spots = []
    for shift in (0, 1):
        where = [jax.random.randint(jax.random.fold_in(stream_key, axis), (), 0, length) for axis, length in enumerate(result.shape)]
        where[longest] = (where[longest] + shift) % result.shape[longest]
        spots.append(tuple(where))
    return result.at[spots[0]].set(low).at[spots[1]].set(high)


def spiked(array, key, source, target, parts, factor):
    owner, partner = [(jnp.arange(array.shape[position]) // (array.shape[position] // parts)).reshape([-1 if axis == position else 1 for axis in range(array.ndim)]) for position in (source, target)]
    chosen = jax.random.permutation(key, parts)[partner]
    strong = (owner == chosen) | (owner == (partner + parts // 2) % parts)
    return jnp.where(strong, factor * array, array)


def levels(stream_key, extent, pieces, low, high):
    gain, own = 1.0, jax.random.fold_in(stream_key, 6)
    for position, shards_of in pieces:
        steps = jnp.exp(jax.random.uniform(jax.random.fold_in(own, position), (shards_of,), jnp.float32, low / len(pieces), high / len(pieces)))
        gain = gain * jnp.repeat(steps, extent[position] // shards_of).reshape([-1 if axis == position else 1 for axis in range(len(extent))])
    return gain


def noise_with(rng, dims, deviation, reach, pieces, heavy, kind=jnp.bfloat16):
    result = deviation * jax.random.normal(rng, dims, jnp.float32)
    if pieces:
        result = result * levels(rng, dims, pieces, -0.22, 0.18)
    return jnp.clip(spiked(result, jax.random.fold_in(rng, 3), *heavy), -reach, reach).astype(kind)


def setup_inputs(seed: int = 0, part: int = 0) -> dict:
    keys = jax.random.split(jax.random.key(seed), 8)
    own_keys = jax.random.split(jax.random.fold_in(keys[7], part), 8)
    pair_density = noise_with(own_keys[0], (PAIRS, NG), 0.033, 0.19921875, ((0, 4), (1, 4)), (0, 1, 4, 2.0))
    band_pairs = draw_band_pairs(jax.random.fold_in(keys[7], 71), part)
    valence = jnp.clip(jax.random.uniform(keys[2], (NV,), jnp.float32, -12.0, -2.0), -12.0, -2.0)
    conduction = jnp.clip(jax.random.uniform(keys[3], (NC,), jnp.float32, 1.0, 8.0), 1.0, 8.0)
    wave_vectors = place_ends(jax.random.randint(own_keys[4], (3, NG), -6, 7), jax.random.fold_in(own_keys[4], 1), -6, 6).astype(jnp.int32)
    momentum = jnp.clip(jax.random.uniform(own_keys[5], (3,), jnp.float32, 0.3, 0.7), 0.3, 0.7)
    guess_scale = jnp.clip(jax.random.uniform(own_keys[6], (NG,), jnp.float32, 0.4, 0.75), 0.4, 0.75)
    return dict(pair_density=pair_density, band_pairs=band_pairs, valence=valence, conduction=conduction, wave_vectors=wave_vectors, momentum=momentum, guess_scale=guess_scale)


def reference(pair_density, band_pairs, valence, conduction, wave_vectors, momentum, guess_scale):
    shifted = wave_vectors.astype(jnp.float32) + momentum[:, None]
    squared_norm = lax.optimization_barrier(jnp.sum(shifted * shifted, axis=0))
    sqrt_v = jnp.sqrt(4.0 * math.pi / squared_norm)
    valence_of = valence[band_pairs[0].astype(jnp.int32)]
    conduction_of = conduction[band_pairs[1].astype(jnp.int32)]
    weight = 4.0 / (valence_of - conduction_of)
    weighted = (weight[:, None] * pair_density.astype(jnp.float32)).astype(jnp.bfloat16)
    chi_zero = jnp.dot(weighted.T, pair_density, preferred_element_type=jnp.float32)
    identity = jnp.eye(chi_zero.shape[0], dtype=jnp.float32)
    epsilon = identity - sqrt_v[:, None] * chi_zero * sqrt_v[None, :]
    guess = guess_scale / jnp.diagonal(epsilon)
    mixed = epsilon * guess[None, :]
    mixed_b = mixed.astype(jnp.bfloat16)
    square = jnp.dot(mixed_b, mixed_b, preferred_element_type=jnp.float32)
    square_b = square.astype(jnp.bfloat16)
    cube = jnp.dot(mixed_b, square_b, preferred_element_type=jnp.float32)
    inverse = guess[:, None] * (4.0 * identity - 6.0 * mixed + 4.0 * square - cube)
    return (epsilon, inverse)
```

```python
import functools
import math

import jax
import jax.numpy as jnp
from jax import lax
from jax.experimental import pallas as pl
from jax.experimental.pallas import tpu as pltpu
from jax.sharding import PartitionSpec as P


def lookup(indices, table):
    levels = jnp.arange(table.shape[0], dtype=jnp.int32)
    picked = indices[:, None] == levels[None, :]
    return jnp.sum(jnp.where(picked, table[None, :], 0.0), axis=1)


def on_device(pair_density, band_pairs, valence, conduction, wave_vectors, momentum, guess_scale):
    column_index = lax.axis_index("col")
    row_index = lax.axis_index("row")
    cols = lax.axis_size("col")
    rows = lax.axis_size("row")
    chips = rows // 2
    depth, height = pair_density.shape
    width = height * rows // cols

    def sibling(value):
        return lax.ppermute(value, "row", [(r ^ 1, r) for r in range(rows)])

    def across(value, k, holders):
        pairs = [
            (c * rows + (r + 2 * k) % rows, c * rows + r) for c in holders for r in range(rows)
        ]
        return lax.ppermute(value, ("col", "row"), pairs)

    def stacked(pieces):
        return jnp.concatenate(pieces, axis=0)

    everyone = range(cols)
    up, down = [pair_density], [pair_density]
    for step in range(1, cols):
        up.append(lax.ppermute(up[-1], "col", [(c - 1, c) for c in range(step, cols)]))
        down.append(lax.ppermute(down[-1], "col", [(c + 1, c) for c in range(cols - step)]))

    def panel_of(upward, downward):
        pieces = [upward[0]]
        for shift in range(1, cols):
            pieces.append(
                jnp.where(column_index >= shift, upward[shift], downward[cols - shift])
            )
        return stacked(pieces)

    near = [panel_of(up, down)]
    for k in range(1, chips):
        own = across(pair_density, k, everyone)
        far_up, far_down = [own], [own]
        for step in range(1, cols):
            far_up.append(across(up[step], k, range(step, cols)))
            far_down.append(across(down[step], k, range(cols - step)))
        near.append(panel_of(far_up, far_down))
    panels = []
    for panel in near:
        panels += [panel, sibling(panel)]
    held = []
    for k in range(chips):
        there = (row_index + 2 * k) % rows
        held += [there, there ^ 1]

    weight_all = 4.0 / (lookup(band_pairs[0], valence) - lookup(band_pairs[1], conduction))
    weight = stacked(
        [
            lax.dynamic_slice_in_dim(weight_all, (column_index - s + cols) % cols * depth, depth, 0)
            for s in range(cols)
        ]
    )
    shifted = wave_vectors.astype(jnp.float32) + momentum[:, None]
    sqrt_all = jnp.sqrt(4.0 * math.pi / jnp.sum(shifted * shifted, axis=0))
    row_first = row_index * height
    column_first = column_index * width
    sqrt_of = [lax.dynamic_slice_in_dim(sqrt_all, h * height, height, 0) for h in held]
    sqrt_cols = lax.dynamic_slice_in_dim(sqrt_all, column_first, width, 0)

    def weigh(panel):
        return (weight[:, None] * panel.astype(jnp.float32)).astype(jnp.bfloat16)

    def chi(left, right):
        return lax.dot_general(
            left, right, (((0,), (0,)), ((), ())), preferred_element_type=jnp.float32
        )

    weighted = [weigh(panel) for panel in near]
    chi_rows = jnp.sum(weighted[0].astype(jnp.float32) * near[0].astype(jnp.float32), axis=0)
    scale_rows = lax.dynamic_slice_in_dim(guess_scale, row_first, height, 0)
    guess_rows = scale_rows / (1.0 - sqrt_of[0] * chi_rows * sqrt_of[0])
    guess_of = []
    for k in range(chips):
        guess_k = guess_rows if k == 0 else across(guess_rows, k, everyone)
        guess_of += [guess_k, sibling(guess_k)]

    def pick(values, axis):
        owner = column_first // height
        chosen = values[0]
        for h, value in zip(held[1:], values[1:]):
            chosen = jnp.where(owner == h, value, chosen)
        return lax.dynamic_slice_in_dim(chosen, column_first % height, width, axis)

    strip_pairs = pick(panels, 1)
    guess_cols = pick(guess_of, 0)

    def delta(row_start, col_start, col_count):
        global_rows = row_start + jnp.arange(height, dtype=jnp.int32)
        global_cols = col_start + jnp.arange(col_count, dtype=jnp.int32)
        return (global_rows[:, None] == global_cols[None, :]).astype(jnp.float32)

    across_panel = []
    for h, panel, sqrt_h, guess_h in zip(held, panels, sqrt_of, guess_of):
        block = delta(row_first, h * height, height) - (
            sqrt_of[0][:, None] * chi(weighted[0], panel) * sqrt_h[None, :]
        )
        across_panel.append((block * guess_h[None, :]).astype(jnp.bfloat16))

    epsilon = None
    strip = []
    for k in range(chips):
        block = delta(held[2 * k] * height, column_first, width) - (
            sqrt_of[2 * k][:, None] * chi(weighted[k], strip_pairs) * sqrt_cols[None, :]
        )
        if k == 0:
            epsilon = block
        mixed_k = (block * guess_cols[None, :]).astype(jnp.bfloat16)
        strip += [mixed_k, sibling(mixed_k)]

    def product(blocks):
        total = None
        for left, right in zip(across_panel, blocks):
            part = jnp.dot(left, right, preferred_element_type=jnp.float32)
            total = part if total is None else total + part
        return total

    parts = 3 if width % 768 == 0 else 1
    size = width // parts
    squares, strips_square = [], []
    for part in range(parts):
        square = product([s[:, part * size : (part + 1) * size] for s in strip])
        square_b = square.astype(jnp.bfloat16)
        squares.append(square)
        blocks = []
        for k in range(chips):
            square_k = square_b if k == 0 else across(square_b, k, everyone)
            blocks += [square_k, sibling(square_k)]
        strips_square.append(blocks)
    inverse = []
    for part in range(parts):
        cube = product(strips_square[part])
        at = slice(part * size, (part + 1) * size)
        identity = delta(row_first, column_first + part * size, size)
        mixed = epsilon[:, at] * guess_cols[None, at]
        inverse.append(
            guess_rows[:, None] * (4.0 * identity - 6.0 * mixed + 4.0 * squares[part] - cube)
        )
    return (epsilon, jnp.concatenate(inverse, axis=1))


MESH = pl.DeviceIdType.MESH
F32, BF16 = jnp.float32, jnp.bfloat16
TILE = 256


def gather_and_iterate(shape_of, pd, pairs, valence, conduction, waves, momentum, scale,
                       v_out, inv_out, v_all, sq_all,
                       rho, total, left, stage, spare, x_chunk,
                       s_row, d_row, t_row, w_row, w_col, columns,
                       load_sem, recv_sem, up_sem, down_sem, x_sem, sib_sem,
                       out_recv, inv_recv, copy_sem, send_sem):
    depth, height, cols, wide, nj, own = shape_of
    total_pairs = depth * cols
    row = lax.axis_index("row")
    z = lax.axis_index("col")
    x, k = row // 2, row % 2
    last = cols - 1
    sibling = {"col": z, "row": 2 * x + 1 - k}
    partner = {"col": z, "row": 2 * (1 - x) + k}
    above = {"col": jnp.minimum(z + 1, last), "row": row}
    below = {"col": jnp.maximum(z - 1, 0), "row": row}
    first_side = z // 2 == x
    lead = z % 2 == k
    mine = row * nj
    theirs = (2 * (1 - x) + k) * nj

    barrier = pltpu.get_barrier_semaphore()
    for who in (sibling, partner):
        pl.semaphore_signal(barrier, inc=1, device_id=who, device_id_type=MESH)

    @pl.when(z < last)
    def _():
        pl.semaphore_signal(barrier, inc=1, device_id=above, device_id_type=MESH)

    @pl.when(z > 0)
    def _():
        pl.semaphore_signal(barrier, inc=1, device_id=below, device_id_type=MESH)

    loads = [
        pltpu.make_async_copy(
            pd.at[:, pl.ds(j * wide, wide)],
            rho.at[mine + j, pl.ds(pl.multiple_of(z * depth, depth), depth), :],
            load_sem.at[j],
        )
        for j in range(nj)
    ]
    for load in loads:
        load.start()
    pl.semaphore_wait(barrier, 4 - jnp.where((z == 0) | (z == last), 1, 0))

    def block(chunk, origin, sem, who):
        part = rho.at[chunk, pl.ds(pl.multiple_of(origin * depth, depth), depth), :]
        return pltpu.make_async_remote_copy(
            src_ref=part,
            dst_ref=part,
            send_sem=sem,
            recv_sem=recv_sem.at[chunk, origin],
            device_id=who,
            device_id_type=MESH,
        )

    def up(j, origin):
        return block(mine + j, origin, up_sem.at[j, origin], above)

    def down(j, origin):
        return block(mine + j, origin, down_sem.at[j, origin], below)

    def over(j, origin):
        return block(mine + j, origin, x_sem.at[j, origin], partner)

    def beside(which, j, origin):
        chunk = (mine if which == 0 else theirs) + j
        return block(chunk, origin, sib_sem.at[which, j, origin], sibling)

    def arrived(chunk, origin):
        block(chunk, origin, up_sem.at[0, 0], sibling).wait_recv()

    late_down = (z == 1) & (x == 0) & (k != 0)
    late_up = (z == last - 1) & (x == last // 2) & (k != last % 2)
    late_over = first_side & jnp.logical_not(lead)

    for j in range(nj):
        loads[j].wait()

        @pl.when((z < last) & jnp.logical_not(late_up))
        def _():
            up(j, z).start()

        @pl.when((z > 0) & jnp.logical_not(late_down))
        def _():
            down(j, z).start()

        over(j, z).start()
        beside(0, j, z).start()

    def eye(n):
        return lax.broadcasted_iota(jnp.int32, (n, n), 0) == lax.broadcasted_iota(
            jnp.int32, (n, n), 1
        )

    def to_column(line):
        n = line.shape[1]
        return jnp.sum(jnp.where(eye(n), jnp.broadcast_to(line, (n, n)), 0.0), axis=1, keepdims=True)

    bands = valence.shape[1]
    levels = lax.broadcasted_iota(jnp.int32, (bands, wide), 0)
    valence_col = to_column(valence[...])
    for part in range(total_pairs // wide):
        at = slice(part * wide, (part + 1) * wide)
        picked = levels == pairs[0:1, at]
        low = jnp.sum(jnp.where(picked, valence_col, 0.0), axis=0, keepdims=True)
        high = jnp.zeros_like(low)
        upper = pairs[1:2, at]
        for band in range(conduction.shape[0]):
            high = jnp.where(upper == band, conduction[band], high)
        weight = 4.0 / (low - high)
        w_row[:, at] = weight
        for piece in range(wide // TILE):
            w_col[part * wide + piece * TILE : part * wide + (piece + 1) * TILE, :] = to_column(
                weight[:, piece * TILE : (piece + 1) * TILE]
            )
    chunks = s_row.shape[0]
    for g in range(chunks):
        at = slice(g * wide, (g + 1) * wide)
        norm = jnp.zeros((1, wide), F32)
        for axis in range(3):
            shifted = waves[axis : axis + 1, at].astype(F32) + momentum[axis]
            norm = norm + shifted * shifted
        s_row[g] = jnp.sqrt(4.0 * math.pi / norm)

    def from_z(distance, j):
        @pl.when(z >= distance)
        def _():
            origin = z - distance
            arrived(mine + j, origin)

            @pl.when((z < last) & jnp.logical_not(late_up))
            def _():
                up(j, origin).start()

            beside(0, j, origin).start()

            @pl.when(jnp.logical_not(late_over & (distance < 3)))
            def _():
                over(j, origin).start()

        @pl.when(z + distance <= last)
        def _():
            origin = z + distance
            arrived(mine + j, origin)

            @pl.when((z > 0) & jnp.logical_not(late_down & (distance < 2)))
            def _():
                down(j, origin).start()

            beside(0, j, origin).start()

            @pl.when(jnp.logical_not(late_over & (distance < 3)))
            def _():
                over(j, origin).start()

    def turn(n):
        ends = jnp.where(z == 0, n, last - n)
        inner = jnp.where(z == 1, (1, 0, 2, 3)[n], (2, 1, 3, 0)[n])
        return jnp.where((z == 0) | (z == last), ends, inner)

    def from_x(n, j):
        arrived(theirs + j, turn(n))
        beside(1, j, turn(n)).start()

    for j in range(nj):
        from_z(1, j)

    @pl.when(late_down)
    def _():
        for j in range(nj):
            down(j, z).start()
        for j in range(nj):
            down(j, z + 1).start()

    @pl.when(late_up)
    def _():
        for j in range(nj):
            up(j, z).start()
        for j in range(nj):
            up(j, z - 1).start()

    eager = jnp.logical_not(first_side) & lead
    for j in range(nj):
        from_x(0, j)

    @pl.when(eager)
    def _():
        for j in range(nj):
            from_x(1, j)

    for j in range(nj):
        from_z(2, j)

    @pl.when(late_up)
    def _():
        for j in range(nj):
            up(j, z - 2).start()

    @pl.when(eager)
    def _():
        for n in (2, 3):
            for j in range(nj):
                from_x(n, j)

    @pl.when(first_side & lead)
    def _():
        for j in range(nj):
            from_z(3, j)

    @pl.when(jnp.logical_not(lead))
    def _():
        for j in range(nj):
            for origin in range(cols):
                arrived(z * nj + j, origin)

    @pl.when(late_over)
    def _():
        for distance in (1, 2):
            for j in range(nj):

                @pl.when(z >= distance)
                def _():
                    over(j, z - distance).start()

                @pl.when(z + distance <= last)
                def _():
                    over(j, z + distance).start()

    for b in range(own // TILE):
        sub = k * (own // TILE) + b
        per = wide // TILE
        chunk = z * nj + sub // per
        lane = pl.multiple_of(sub % per * TILE, TILE)

        def turned(p, diagonal):
            at = pl.ds(pl.multiple_of(p * TILE, TILE), TILE)
            piece = rho[chunk, at, pl.ds(lane, TILE)].astype(F32)
            heavy = (w_col[at, :] * piece).astype(BF16).astype(F32)
            left[pl.ds(b * TILE, TILE), at] = heavy.T.astype(BF16)
            return diagonal + jnp.sum(heavy * piece, axis=0, keepdims=True)

        diagonal = lax.fori_loop(0, total_pairs // TILE, turned, jnp.zeros((1, TILE), F32))
        s_part = s_row[chunk, :, pl.ds(lane, TILE)]
        g_part = scale[chunk, :, pl.ds(lane, TILE)]
        rows_at = slice(b * TILE, (b + 1) * TILE)
        columns[rows_at, 0:1] = to_column(s_part)
        columns[rows_at, 1:2] = to_column(g_part / (1.0 - s_part * diagonal * s_part))
        columns[rows_at, 2:3] = to_column(g_part.astype(BF16).astype(F32))
        columns[rows_at, 3:4] = jnp.zeros((TILE, 1), F32)

    total[...] = jnp.zeros_like(total)
    c_first = z * height + k * own

    def on_diagonal(g, m):
        rows_of = lax.broadcasted_iota(jnp.int32, (TILE, wide), 0) + (c_first + m * TILE)
        cols_of = lax.broadcasted_iota(jnp.int32, (TILE, wide), 1) + g * wide
        return rows_of == cols_of

    def project(m, g):
        return jnp.dot(
            left[m * TILE : (m + 1) * TILE, :], rho[g], preferred_element_type=F32
        )

    def accumulate(g):
        values = x_chunk[...]
        for p in range(total_pairs // wide):
            at = slice(p * wide, (p + 1) * wide)
            total[:, at] += lax.dot_general(
                values,
                rho[g, at, :],
                (((1,), (1,)), ((), ())),
                preferred_element_type=F32,
            )

    def out_copies(source, target, landed, j):
        there = target.at[j, pl.ds(pl.multiple_of(k * own, own), own), :]
        near = pltpu.make_async_copy(source, there, copy_sem.at[1])
        far = pltpu.make_async_remote_copy(
            src_ref=source,
            dst_ref=there,
            send_sem=send_sem.at[0],
            recv_sem=landed.at[j],
            device_id=sibling,
            device_id_type=MESH,
        )
        return near, far

    def chunk_at(i):
        other = (2 * x + 1 - z % 2) * nj + i - 3
        across = (2 * (1 - x) + (i - 6) % 2) * nj + (i - 6) // 2
        near = jnp.where(i < 6, other, across)
        both = (2 * x + (i - 3) % 2) * nj + (i - 3) // 2
        rest = (2 * (1 - x) + 1 - z % 2) * nj + i - 9
        far = jnp.where(i < 9, both, rest)
        return jnp.where(i < 3, z * nj + i, jnp.where(first_side, near, far))

    def first_pass(i, carry):
        for n in (1, 2, 3):
            base = jnp.where(first_side, 3 * (n - 1), 3 * n)
            stride = jnp.where(first_side & (n == 3), 2, 1)
            j = (i - base) // stride

            @pl.when(
                jnp.logical_not(eager) & (i >= base) & ((i - base) % stride == 0) & (j < nj)
            )
            def _():
                from_x(n, j)

        stride = jnp.where(first_side, 1, 2)
        jz = (i - 3) // stride

        @pl.when(
            jnp.logical_not(first_side & lead)
            & (i >= 3)
            & ((i - 3) % stride == 0)
            & (jz < nj)
        )
        def _():
            from_z(3, jz)

        g = chunk_at(i)
        panel = g // nj

        @pl.when((i >= 3) & (panel % 2 != k))
        def _():
            for origin in range(cols):
                arrived(g, origin)

        def weigh(p, diagonal):
            at = pl.ds(pl.multiple_of(p * TILE, TILE), TILE)
            piece = rho[g, at, :].astype(F32)
            heavy = (w_col[at, :] * piece).astype(BF16).astype(F32)
            return diagonal + jnp.sum(heavy * piece, axis=0, keepdims=True)

        diagonal = lax.fori_loop(0, total_pairs // TILE, weigh, jnp.zeros((1, wide), F32))
        s_g, scale_g = s_row[g], scale[g]
        d_g = scale_g / (1.0 - s_g * diagonal * s_g)
        d_row[g] = d_g
        t_row[g] = d_g + (scale_g.astype(BF16).astype(F32) - scale_g)
        for m in range(own // TILE):
            rows_at = slice(m * TILE, (m + 1) * TILE)
            v = project(m, g) * columns[rows_at, 0:1] * s_g
            stage[rows_at, :] = v
            off = jnp.where(on_diagonal(g, m), 0.0, -v * columns[rows_at, 1:2])
            off = off.astype(BF16).astype(F32)
            x_chunk[rows_at, :] = (off * (s_g * d_g)).astype(BF16)
        keep = pltpu.make_async_copy(stage, v_all.at[g], copy_sem.at[0])
        keep.start()
        near, far = out_copies(stage, v_out, out_recv, g % nj)

        @pl.when(panel == row)
        def _():
            near.start()

        @pl.when(panel == 2 * x + 1 - k)
        def _():
            far.start()

        accumulate(g)
        keep.wait()

        @pl.when(panel == row)
        def _():
            near.wait()

        @pl.when(panel == 2 * x + 1 - k)
        def _():
            far.wait_send()

        return carry

    lax.fori_loop(0, chunks, first_pass, 0)

    def close():
        for p in range(total_pairs // wide):
            at = slice(p * wide, (p + 1) * wide)
            left[:, at] = (total[:, at] * w_row[:, at]).astype(BF16)

    close()
    total[...] = jnp.zeros_like(total)

    def second_pass(g, carry):
        fetch = pltpu.make_async_copy(v_all.at[g], spare, copy_sem.at[0])
        fetch.start()
        fetch.wait()
        s_g, d_g, t_g = s_row[g], d_row[g], t_row[g]
        for m in range(own // TILE):
            rows_at = slice(m * TILE, (m + 1) * TILE)
            y = project(m, g) * s_g
            here = on_diagonal(g, m)
            t_c = columns[rows_at, 2:3]
            off = jnp.where(here, 0.0, -spare[rows_at, :] * columns[rows_at, 1:2])
            off = off.astype(BF16).astype(F32)
            square = (t_c + t_g) * off - y + jnp.where(here, t_c * t_c, 0.0)
            stage[rows_at, :] = square
            rounded = square.astype(BF16).astype(F32)
            columns[rows_at, 3:4] += jnp.sum(
                jnp.where(here, rounded, 0.0), axis=1, keepdims=True
            )
            rounded = jnp.where(here, 0.0, rounded)
            x_chunk[rows_at, :] = (rounded * (s_g * d_g)).astype(BF16)
        keep = pltpu.make_async_copy(stage, sq_all.at[g % (2 * nj)], copy_sem.at[1])
        half = g // (2 * nj) == x

        @pl.when(half)
        def _():
            keep.start()

        accumulate(g)

        @pl.when(half)
        def _():
            keep.wait()

        return carry

    lax.fori_loop(0, chunks, second_pass, 0)
    close()

    def third_pass(j, carry):
        for side in range(2):
            panel = 2 * x + (1 - k if side == 0 else k)
            g = panel * nj + j
            source = stage if side == 0 else spare
            near, far = out_copies(source, inv_out, inv_recv, j)
            first = pltpu.make_async_copy(
                v_all.at[g], total.at[:, pl.ds(0, wide)], copy_sem.at[0]
            )
            second = pltpu.make_async_copy(
                sq_all.at[g % (2 * nj)], total.at[:, pl.ds(wide, wide)], copy_sem.at[2]
            )
            first.start()
            second.start()

            @pl.when(j > 0)
            def _():
                if side == 0:
                    far.wait_send()
                else:
                    near.wait()

            first.wait()
            second.wait()
            s_g, d_g, t_g = s_row[g], d_row[g], t_row[g]
            for m in range(own // TILE):
                rows_at = slice(m * TILE, (m + 1) * TILE)
                y = project(m, g) * s_g
                here = on_diagonal(g, m)
                d_c, t_c, q_c = (columns[rows_at, n : n + 1] for n in (1, 2, 3))
                v = total[rows_at, 0:wide]
                square = total[rows_at, wide : 2 * wide]
                mixed = jnp.where(here, 1.0 - v, -v) * d_c
                off = jnp.where(here, t_c, mixed.astype(BF16).astype(F32))
                rounded = jnp.where(here, 0.0, square.astype(BF16).astype(F32))
                cube = q_c * off + t_g * rounded - y
                source[rows_at, :] = d_g * (
                    jnp.where(here, 4.0, 0.0) - 6.0 * mixed + 4.0 * square - cube
                )
            if side == 0:
                far.start()
            else:
                near.start()
        return carry

    lax.fori_loop(0, nj, third_pass, 0)
    near, far = out_copies(stage, inv_out, inv_recv, 0)
    far.wait_send()
    near, far = out_copies(spare, inv_out, inv_recv, 0)
    near.wait()

    for j in range(nj):
        for landed, target in ((out_recv, v_out), (inv_recv, inv_out)):
            pltpu.make_async_remote_copy(
                src_ref=stage,
                dst_ref=target.at[j, pl.ds(pl.multiple_of((1 - k) * own, own), own), :],
                send_sem=send_sem.at[0],
                recv_sem=landed.at[j],
                device_id=sibling,
                device_id_type=MESH,
            ).wait_recv()

        for origin in range(cols):
            over(j, origin).wait_send()
            beside(0, j, origin).wait_send()
            beside(1, j, origin).wait_send()

            @pl.when((z < last) & (origin <= z))
            def _():
                up(j, origin).wait_send()

            @pl.when((z > 0) & (origin >= z))
            def _():
                down(j, origin).wait_send()


def in_one_kernel(pair_density, band_pairs, valence, conduction, wave_vectors, momentum, guess_scale):
    cols = lax.axis_size("col")
    rows = lax.axis_size("row")
    depth, height = pair_density.shape
    width = height * rows // cols
    wide = 2 * TILE
    nj = height // wide
    own = width // 2
    chunks = rows * nj
    pairs = depth * cols
    vm = pl.BlockSpec(memory_space=pltpu.VMEM)
    sm = pl.BlockSpec(memory_space=pltpu.SMEM)
    hbm = pl.BlockSpec(memory_space=pl.ANY)
    dma = pltpu.SemaphoreType.DMA
    body = functools.partial(gather_and_iterate, (depth, height, cols, wide, nj, own))
    v_turned, inverse_turned, _, _ = pl.pallas_call(
        body,
        out_shape=(
            jax.ShapeDtypeStruct((nj, width, wide), F32),
            jax.ShapeDtypeStruct((nj, width, wide), F32),
            jax.ShapeDtypeStruct((chunks, own, wide), F32),
            jax.ShapeDtypeStruct((2 * nj, own, wide), F32),
        ),
        in_specs=[hbm, vm, vm, sm, vm, sm, vm],
        out_specs=(hbm,) * 4,
        scratch_shapes=[
            pltpu.VMEM((chunks, pairs, wide), BF16),
            pltpu.VMEM((own, pairs), F32),
            pltpu.VMEM((own, pairs), BF16),
            pltpu.VMEM((own, wide), F32),
            pltpu.VMEM((own, wide), F32),
            pltpu.VMEM((own, wide), BF16),
            pltpu.VMEM((chunks, 1, wide), F32),
            pltpu.VMEM((chunks, 1, wide), F32),
            pltpu.VMEM((chunks, 1, wide), F32),
            pltpu.VMEM((1, pairs), F32),
            pltpu.VMEM((pairs, 1), F32),
            pltpu.VMEM((own, 128), F32),
            dma((nj,)),
            dma((chunks, cols)),
            dma((nj, cols)),
            dma((nj, cols)),
            dma((nj, cols)),
            dma((2, nj, cols)),
            dma((nj,)),
            dma((nj,)),
            dma((3,)),
            dma((1,)),
        ],
        compiler_params=pltpu.CompilerParams(
            collective_id=0, has_side_effects=True, vmem_limit_bytes=67043328
        ),
    )(
        pair_density,
        band_pairs,
        valence.reshape(1, -1),
        conduction,
        wave_vectors,
        momentum,
        guess_scale.reshape(chunks, 1, wide),
    )

    def back(value):
        return jnp.swapaxes(value, 1, 2).reshape(height, width)

    rows_of = lax.axis_index("row") * height + lax.broadcasted_iota(jnp.int32, (height, width), 0)
    cols_of = lax.axis_index("col") * width + lax.broadcasted_iota(jnp.int32, (height, width), 1)
    epsilon = (rows_of == cols_of).astype(F32) - back(v_turned)
    return (epsilon, back(inverse_turned))


def solution(mesh):
    placed = (P(("pb", "col"), "row"), P(), P(), P(), P(None, "pb"), P("pb"), P("pb"))
    square_mesh = mesh.shape["row"] == 4 and mesh.shape["col"] == 4
    return jax.shard_map(
        in_one_kernel if square_mesh else on_device,
        mesh=mesh,
        in_specs=placed,
        out_specs=(P(("pb", "row"), "col"), P(("pb", "row"), "col")),
        check_vma=False,
    )
```

```python
import functools
import math

import jax
import jax.numpy as jnp
from jax import lax
from jax.experimental import pallas as pl
from jax.experimental.pallas import tpu as pltpu
from jax.sharding import PartitionSpec as P


def lookup(indices, table):
    levels = jnp.arange(table.shape[0], dtype=jnp.int32)
    picked = indices[:, None] == levels[None, :]
    return jnp.sum(jnp.where(picked, table[None, :], 0.0), axis=1)


def on_device(pair_density, band_pairs, valence, conduction, wave_vectors, momentum, guess_scale):
    column_index = lax.axis_index("col")
    row_index = lax.axis_index("row")
    cols = lax.axis_size("col")
    rows = lax.axis_size("row")
    chips = rows // 2
    depth, height = pair_density.shape
    width = height * rows // cols

    def sibling(value):
        return lax.ppermute(value, "row", [(r ^ 1, r) for r in range(rows)])

    def across(value, k, holders):
        pairs = [
            (c * rows + (r + 2 * k) % rows, c * rows + r) for c in holders for r in range(rows)
        ]
        return lax.ppermute(value, ("col", "row"), pairs)

    def stacked(pieces):
        return jnp.concatenate(pieces, axis=0)

    everyone = range(cols)
    up, down = [pair_density], [pair_density]
    for step in range(1, cols):
        up.append(lax.ppermute(up[-1], "col", [(c - 1, c) for c in range(step, cols)]))
        down.append(lax.ppermute(down[-1], "col", [(c + 1, c) for c in range(cols - step)]))

    def panel_of(upward, downward):
        pieces = [upward[0]]
        for shift in range(1, cols):
            pieces.append(
                jnp.where(column_index >= shift, upward[shift], downward[cols - shift])
            )
        return stacked(pieces)

    near = [panel_of(up, down)]
    for k in range(1, chips):
        own = across(pair_density, k, everyone)
        far_up, far_down = [own], [own]
        for step in range(1, cols):
            far_up.append(across(up[step], k, range(step, cols)))
            far_down.append(across(down[step], k, range(cols - step)))
        near.append(panel_of(far_up, far_down))
    panels = []
    for panel in near:
        panels += [panel, sibling(panel)]
    held = []
    for k in range(chips):
        there = (row_index + 2 * k) % rows
        held += [there, there ^ 1]

    weight_all = 4.0 / (lookup(band_pairs[0], valence) - lookup(band_pairs[1], conduction))
    weight = stacked(
        [
            lax.dynamic_slice_in_dim(weight_all, (column_index - s + cols) % cols * depth, depth, 0)
            for s in range(cols)
        ]
    )
    shifted = wave_vectors.astype(jnp.float32) + momentum[:, None]
    sqrt_all = jnp.sqrt(4.0 * math.pi / jnp.sum(shifted * shifted, axis=0))
    row_first = row_index * height
    column_first = column_index * width
    sqrt_of = [lax.dynamic_slice_in_dim(sqrt_all, h * height, height, 0) for h in held]
    sqrt_cols = lax.dynamic_slice_in_dim(sqrt_all, column_first, width, 0)

    def weigh(panel):
        return (weight[:, None] * panel.astype(jnp.float32)).astype(jnp.bfloat16)

    def chi(left, right):
        return lax.dot_general(
            left, right, (((0,), (0,)), ((), ())), preferred_element_type=jnp.float32
        )

    weighted = [weigh(panel) for panel in near]
    chi_rows = jnp.sum(weighted[0].astype(jnp.float32) * near[0].astype(jnp.float32), axis=0)
    scale_rows = lax.dynamic_slice_in_dim(guess_scale, row_first, height, 0)
    guess_rows = scale_rows / (1.0 - sqrt_of[0] * chi_rows * sqrt_of[0])
    guess_of = []
    for k in range(chips):
        guess_k = guess_rows if k == 0 else across(guess_rows, k, everyone)
        guess_of += [guess_k, sibling(guess_k)]

    def pick(values, axis):
        owner = column_first // height
        chosen = values[0]
        for h, value in zip(held[1:], values[1:]):
            chosen = jnp.where(owner == h, value, chosen)
        return lax.dynamic_slice_in_dim(chosen, column_first % height, width, axis)

    strip_pairs = pick(panels, 1)
    guess_cols = pick(guess_of, 0)

    def delta(row_start, col_start, col_count):
        global_rows = row_start + jnp.arange(height, dtype=jnp.int32)
        global_cols = col_start + jnp.arange(col_count, dtype=jnp.int32)
        return (global_rows[:, None] == global_cols[None, :]).astype(jnp.float32)

    across_panel = []
    for h, panel, sqrt_h, guess_h in zip(held, panels, sqrt_of, guess_of):
        block = delta(row_first, h * height, height) - (
            sqrt_of[0][:, None] * chi(weighted[0], panel) * sqrt_h[None, :]
        )
        across_panel.append((block * guess_h[None, :]).astype(jnp.bfloat16))

    epsilon = None
    strip = []
    for k in range(chips):
        block = delta(held[2 * k] * height, column_first, width) - (
            sqrt_of[2 * k][:, None] * chi(weighted[k], strip_pairs) * sqrt_cols[None, :]
        )
        if k == 0:
            epsilon = block
        mixed_k = (block * guess_cols[None, :]).astype(jnp.bfloat16)
        strip += [mixed_k, sibling(mixed_k)]

    def product(blocks):
        total = None
        for left, right in zip(across_panel, blocks):
            part = jnp.dot(left, right, preferred_element_type=jnp.float32)
            total = part if total is None else total + part
        return total

    parts = 3 if width % 768 == 0 else 1
    size = width // parts
    squares, strips_square = [], []
    for part in range(parts):
        square = product([s[:, part * size : (part + 1) * size] for s in strip])
        square_b = square.astype(jnp.bfloat16)
        squares.append(square)
        blocks = []
        for k in range(chips):
            square_k = square_b if k == 0 else across(square_b, k, everyone)
            blocks += [square_k, sibling(square_k)]
        strips_square.append(blocks)
    inverse = []
    for part in range(parts):
        cube = product(strips_square[part])
        at = slice(part * size, (part + 1) * size)
        identity = delta(row_first, column_first + part * size, size)
        mixed = epsilon[:, at] * guess_cols[None, at]
        inverse.append(
            guess_rows[:, None] * (4.0 * identity - 6.0 * mixed + 4.0 * squares[part] - cube)
        )
    return (epsilon, jnp.concatenate(inverse, axis=1))


MESH = pl.DeviceIdType.MESH
F32, BF16 = jnp.float32, jnp.bfloat16
TILE, SLIM, FEW = 256, 64, 32


def gather_and_iterate(shape_of, pd, pairs, valence, conduction, waves, momentum, scale,
                       e_out, inv_out, e_all, sq_all,
                       rho, total, left, staged, x_chunk,
                       s_row, d_row, t_row, w_row, w_col, columns,
                       load_sem, recv_sem, up_sem, down_sem, x_sem, sib_sem,
                       out_recv, inv_recv, copy_sem, send_sem):
    depth, height, cols, wide, nj, own = shape_of
    stage, spare = staged.at[0], staged.at[1]
    total_pairs = depth * cols
    row = lax.axis_index("row")
    z = lax.axis_index("col")
    x, k = row // 2, row % 2
    last = cols - 1
    sibling = {"col": z, "row": 2 * x + 1 - k}
    partner = {"col": z, "row": 2 * (1 - x) + k}
    above = {"col": jnp.minimum(z + 1, last), "row": row}
    below = {"col": jnp.maximum(z - 1, 0), "row": row}
    first_side = z // 2 == x
    lead = z % 2 == k
    mine = row * nj
    theirs = (2 * (1 - x) + k) * nj

    barrier = pltpu.get_barrier_semaphore()
    for who in (sibling, partner):
        pl.semaphore_signal(barrier, inc=1, device_id=who, device_id_type=MESH)

    @pl.when(z < last)
    def _():
        pl.semaphore_signal(barrier, inc=1, device_id=above, device_id_type=MESH)

    @pl.when(z > 0)
    def _():
        pl.semaphore_signal(barrier, inc=1, device_id=below, device_id_type=MESH)

    loads = [
        pltpu.make_async_copy(
            pd.at[:, pl.ds(j * wide, wide)],
            rho.at[mine + j, pl.ds(pl.multiple_of(z * depth, depth), depth), :],
            load_sem.at[j],
        )
        for j in range(nj)
    ]
    for load in loads:
        load.start()
    pl.semaphore_wait(barrier, 4 - jnp.where((z == 0) | (z == last), 1, 0))

    def block(chunk, origin, sem, who):
        part = rho.at[chunk, pl.ds(pl.multiple_of(origin * depth, depth), depth), :]
        return pltpu.make_async_remote_copy(
            src_ref=part,
            dst_ref=part,
            send_sem=sem,
            recv_sem=recv_sem.at[chunk, origin],
            device_id=who,
            device_id_type=MESH,
        )

    def up(j, origin):
        return block(mine + j, origin, up_sem.at[j, origin], above)

    def down(j, origin):
        return block(mine + j, origin, down_sem.at[j, origin], below)

    def over(j, origin):
        return block(mine + j, origin, x_sem.at[j, origin], partner)

    def beside(which, j, origin):
        chunk = (mine if which == 0 else theirs) + j
        return block(chunk, origin, sib_sem.at[which, j, origin], sibling)

    def arrived(chunk, origin):
        block(chunk, origin, up_sem.at[0, 0], sibling).wait_recv()

    late_down = (z == 1) & (x == 0) & (k != 0)
    late_up = (z == last - 1) & (x == last // 2) & (k != last % 2)
    late_over = first_side & jnp.logical_not(lead)

    for j in range(nj):
        loads[j].wait()

        @pl.when((z < last) & jnp.logical_not(late_up))
        def _():
            up(j, z).start()

        @pl.when((z > 0) & jnp.logical_not(late_down))
        def _():
            down(j, z).start()

        over(j, z).start()
        beside(0, j, z).start()

    def eye(n):
        return lax.broadcasted_iota(jnp.int32, (n, n), 0) == lax.broadcasted_iota(
            jnp.int32, (n, n), 1
        )

    def to_column(line):
        n = line.shape[1]
        return jnp.sum(jnp.where(eye(n), jnp.broadcast_to(line, (n, n)), 0.0), axis=1, keepdims=True)

    bands = valence.shape[1]
    levels = lax.broadcasted_iota(jnp.int32, (bands, wide), 0)
    valence_col = to_column(valence[...])
    w_col[...] = jnp.zeros_like(w_col)
    for part in range(total_pairs // wide):
        at = slice(part * wide, (part + 1) * wide)
        picked = levels == pairs[0:1, at]
        low = jnp.sum(jnp.where(picked, valence_col, 0.0), axis=0, keepdims=True)
        high = jnp.zeros_like(low)
        upper = pairs[1:2, at]
        for band in range(conduction.shape[0]):
            high = jnp.where(upper == band, conduction[band], high)
        weight = 4.0 / (low - high)
        w_row[:, at] = weight
        for piece in range(wide // TILE):
            first = part * wide + piece * TILE
            w_col[first % depth : first % depth + TILE, first // depth : first // depth + 1] = (
                to_column(weight[:, piece * TILE : (piece + 1) * TILE])
            )
    chunks = s_row.shape[0]
    for g in range(chunks):
        at = slice(g * wide, (g + 1) * wide)
        norm = jnp.zeros((1, wide), F32)
        for axis in range(3):
            shifted = waves[axis : axis + 1, at].astype(F32) + momentum[axis]
            norm = norm + shifted * shifted
        s_row[g] = jnp.sqrt(4.0 * math.pi / norm)
        d_row[g] = jnp.zeros((1, wide), F32)

    def weights_at(start, count):
        lanes = w_col[pl.ds(pl.multiple_of(start % depth, count), count), :]
        at = lax.broadcasted_iota(jnp.int32, lanes.shape, 1) == start // depth
        return jnp.sum(jnp.where(at, lanes, 0.0), axis=1, keepdims=True)

    def add_diagonal(chunk, start, steps):
        def weigh(p, diagonal):
            at = pl.ds(pl.multiple_of(start + p * SLIM, SLIM), SLIM)
            piece = rho[chunk, at, :].astype(F32)
            heavy = (weights_at(start + p * SLIM, SLIM) * piece).astype(BF16).astype(F32)
            return diagonal + jnp.sum(heavy * piece, axis=0, keepdims=True)

        d_row[chunk] = lax.fori_loop(0, steps, weigh, d_row[chunk])

    per_block = depth // SLIM
    for j in range(nj):
        add_diagonal(mine + j, z * depth, per_block)

    def from_z(distance, j):
        @pl.when(z >= distance)
        def _():
            origin = z - distance
            arrived(mine + j, origin)

            @pl.when((z < last) & jnp.logical_not(late_up))
            def _():
                up(j, origin).start()

            beside(0, j, origin).start()

            @pl.when(jnp.logical_not(late_over & (distance < 3)))
            def _():
                over(j, origin).start()

            add_diagonal(mine + j, origin * depth, per_block)

        @pl.when(z + distance <= last)
        def _():
            origin = z + distance
            arrived(mine + j, origin)

            @pl.when((z > 0) & jnp.logical_not(late_down & (distance < 2)))
            def _():
                down(j, origin).start()

            beside(0, j, origin).start()

            @pl.when(jnp.logical_not(late_over & (distance < 3)))
            def _():
                over(j, origin).start()

            add_diagonal(mine + j, origin * depth, per_block)

    def turn(n):
        ends = jnp.where(z == 0, n, last - n)
        inner = jnp.where(z == 1, (1, 0, 2, 3)[n], (2, 1, 3, 0)[n])
        return jnp.where((z == 0) | (z == last), ends, inner)

    def from_x(n, j):
        arrived(theirs + j, turn(n))
        beside(1, j, turn(n)).start()
        add_diagonal(theirs + j, turn(n) * depth, per_block)

    for j in range(nj):
        from_z(1, j)

    @pl.when(late_down)
    def _():
        for j in range(nj):
            down(j, z).start()
        for j in range(nj):
            down(j, z + 1).start()

    @pl.when(late_up)
    def _():
        for j in range(nj):
            up(j, z).start()
        for j in range(nj):
            up(j, z - 1).start()

    eager = jnp.logical_not(first_side) & lead
    for j in range(nj):
        from_x(0, j)

    @pl.when(eager)
    def _():
        for j in range(nj):
            from_x(1, j)

    for j in range(nj):
        from_z(2, j)

    @pl.when(late_up)
    def _():
        for j in range(nj):
            up(j, z - 2).start()

    @pl.when(eager)
    def _():
        for n in (2, 3):
            for j in range(nj):
                from_x(n, j)

    @pl.when(first_side & lead)
    def _():
        for j in range(nj):
            from_z(3, j)

    @pl.when(jnp.logical_not(lead))
    def _():
        for j in range(nj):
            for origin in range(cols):
                arrived(z * nj + j, origin)

    @pl.when(late_over)
    def _():
        for distance in (1, 2):
            for j in range(nj):

                @pl.when(z >= distance)
                def _():
                    over(j, z - distance).start()

                @pl.when(z + distance <= last)
                def _():
                    over(j, z + distance).start()

    for b in range(own // TILE):
        sub = k * (own // TILE) + b
        per = wide // TILE
        chunk = z * nj + sub // per
        lane = pl.multiple_of(sub % per * TILE, TILE)

        def turned(p, diagonal):
            at = pl.ds(pl.multiple_of(p * TILE, TILE), TILE)
            piece = rho[chunk, at, pl.ds(lane, TILE)].astype(F32)
            heavy = (weights_at(p * TILE, TILE) * piece).astype(BF16).astype(F32)
            left[pl.ds(b * TILE, TILE), at] = heavy.T.astype(BF16)
            return diagonal + jnp.sum(heavy * piece, axis=0, keepdims=True)

        diagonal = lax.fori_loop(0, total_pairs // TILE, turned, jnp.zeros((1, TILE), F32))
        s_part = s_row[chunk, :, pl.ds(lane, TILE)]
        g_part = scale[chunk, :, pl.ds(lane, TILE)]
        rows_at = slice(b * TILE, (b + 1) * TILE)
        columns[rows_at, 0:1] = to_column(s_part)
        columns[rows_at, 1:2] = to_column(g_part / (1.0 - s_part * diagonal * s_part))
        columns[rows_at, 2:3] = to_column(g_part.astype(BF16).astype(F32))
        columns[rows_at, 3:4] = jnp.zeros((TILE, 1), F32)

    total[...] = jnp.zeros_like(total)
    c_first = z * height + k * own

    def on_diagonal(g, first):
        rows_of = lax.broadcasted_iota(jnp.int32, (FEW, wide), 0) + (c_first + first)
        cols_of = lax.broadcasted_iota(jnp.int32, (FEW, wide), 1) + g * wide
        return rows_of == cols_of

    def project(target, g):
        for m in range(own // TILE):
            rows_at = slice(m * TILE, (m + 1) * TILE)
            target[rows_at, :] = jnp.dot(left[rows_at, :], rho[g], preferred_element_type=F32)
            for few in range(TILE // FEW):
                first = m * TILE + few * FEW
                yield slice(first, first + FEW), on_diagonal(g, first)

    def accumulate(g):
        for p in range(total_pairs // wide):
            at = slice(p * wide, (p + 1) * wide)
            total[:, at] += lax.dot_general(
                x_chunk[...],
                rho[g, at, :],
                (((1,), (1,)), ((), ())),
                preferred_element_type=F32,
            )

    def out_copies(source, target, landed, j):
        there = target.at[j, pl.ds(pl.multiple_of(k * own, own), own), :]
        near = pltpu.make_async_copy(source, there, copy_sem.at[1])
        far = pltpu.make_async_remote_copy(
            src_ref=source,
            dst_ref=there,
            send_sem=send_sem.at[0],
            recv_sem=landed.at[j],
            device_id=sibling,
            device_id_type=MESH,
        )
        return near, far

    def chunk_at(i):
        other = (2 * x + 1 - z % 2) * nj + i - 3
        across = (2 * (1 - x) + (i - 6) % 2) * nj + (i - 6) // 2
        near = jnp.where(i < 6, other, across)
        both = (2 * x + (i - 3) % 2) * nj + (i - 3) // 2
        rest = (2 * (1 - x) + 1 - z % 2) * nj + i - 9
        far = jnp.where(i < 9, both, rest)
        return jnp.where(i < 3, z * nj + i, jnp.where(first_side, near, far))

    def first_pass(i, carry):
        for n in (1, 2, 3):
            base = jnp.where(first_side, 3 * (n - 1), 3 * n)
            stride = jnp.where(first_side & (n == 3), 2, 1)
            j = (i - base) // stride

            @pl.when(
                jnp.logical_not(eager) & (i >= base) & ((i - base) % stride == 0) & (j < nj)
            )
            def _():
                from_x(n, j)

        stride = jnp.where(first_side, 1, 2)
        jz = (i - 3) // stride

        @pl.when(
            jnp.logical_not(first_side & lead)
            & (i >= 3)
            & ((i - 3) % stride == 0)
            & (jz < nj)
        )
        def _():
            from_z(3, jz)

        g = chunk_at(i)
        panel = g // nj

        @pl.when((i >= 3) & (panel % 2 != k))
        def _():
            for origin in range(cols):
                arrived(g, origin)

        @pl.when(panel % 2 != k)
        def _():
            add_diagonal(g, 0, total_pairs // SLIM)

        diagonal = d_row[g]
        s_g, scale_g = s_row[g], scale[g]
        d_g = scale_g / (1.0 - s_g * diagonal * s_g)
        d_row[g] = d_g
        t_row[g] = d_g + (scale_g.astype(BF16).astype(F32) - scale_g)
        for rows_at, here in project(stage, g):
            v = stage[rows_at, :] * columns[rows_at, 0:1] * s_g
            value = jnp.where(here, 1.0, 0.0) - v
            stage[rows_at, :] = value
            off = jnp.where(here, 0.0, value * columns[rows_at, 1:2])
            off = off.astype(BF16).astype(F32)
            x_chunk[rows_at, :] = (off * (s_g * d_g)).astype(BF16)
        keep = pltpu.make_async_copy(stage, e_all.at[g], copy_sem.at[0])
        keep.start()
        near, far = out_copies(stage, e_out, out_recv, g % nj)

        @pl.when(panel == row)
        def _():
            near.start()

        @pl.when(panel == 2 * x + 1 - k)
        def _():
            far.start()

        accumulate(g)
        keep.wait()

        @pl.when(panel == row)
        def _():
            near.wait()

        @pl.when(panel == 2 * x + 1 - k)
        def _():
            far.wait_send()

        return carry

    lax.fori_loop(0, chunks, first_pass, 0)

    def close():
        def scaled(r, carry):
            at = pl.ds(pl.multiple_of(r * 16, 16), 16)
            left[at, :] = (total[at, :] * w_row[...]).astype(BF16)
            return carry

        lax.fori_loop(0, own // 16, scaled, 0)

    close()
    total[...] = jnp.zeros_like(total)

    def fetch(g):
        return pltpu.make_async_copy(e_all.at[g], spare, copy_sem.at[0])

    fetch(0).start()

    def second_pass(g, carry):
        fetch(g).wait()
        s_g, d_g, t_g = s_row[g], d_row[g], t_row[g]
        for rows_at, here in project(stage, g):
            y = stage[rows_at, :] * s_g
            t_c = columns[rows_at, 2:3]
            off = jnp.where(here, 0.0, spare[rows_at, :] * columns[rows_at, 1:2])
            off = off.astype(BF16).astype(F32)
            square = (t_c + t_g) * off - y + jnp.where(here, t_c * t_c, 0.0)
            stage[rows_at, :] = square
            rounded = square.astype(BF16).astype(F32)
            columns[rows_at, 3:4] += jnp.sum(
                jnp.where(here, rounded, 0.0), axis=1, keepdims=True
            )
            rounded = jnp.where(here, 0.0, rounded)
            x_chunk[rows_at, :] = (rounded * (s_g * d_g)).astype(BF16)

        @pl.when(g + 1 < chunks)
        def _():
            fetch(g + 1).start()

        keep = pltpu.make_async_copy(stage, sq_all.at[g % (2 * nj)], copy_sem.at[1])
        half = g // (2 * nj) == x

        @pl.when(half)
        def _():
            keep.start()

        accumulate(g)

        @pl.when(half)
        def _():
            keep.wait()

        return carry

    lax.fori_loop(0, chunks, second_pass, 0)
    close()

    def operands(n):
        j, side = n // 2, n % 2
        g = (2 * x + (1 - k) * (1 - side) + k * side) * nj + j
        at = [pl.ds(pl.multiple_of((2 * side + m) * wide, wide), wide) for m in range(2)]
        sources = e_all.at[g], sq_all.at[g % (2 * nj)]
        return [
            pltpu.make_async_copy(source, total.at[:, at[m]], copy_sem.at[2 + 2 * side + m])
            for m, source in enumerate(sources)
        ]

    for copy in operands(0):
        copy.start()

    def third_pass(n, carry):
        j, side = n // 2, n % 2
        g = (2 * x + (1 - k) * (1 - side) + k * side) * nj + j
        near, far = out_copies(staged.at[side], inv_out, inv_recv, j)
        for copy in operands(n):
            copy.wait()

        @pl.when(n + 1 < 2 * nj)
        def _():
            for copy in operands(n + 1):
                copy.start()

        @pl.when((n > 1) & (side == 0))
        def _():
            far.wait_send()

        @pl.when((n > 1) & (side == 1))
        def _():
            near.wait()

        s_g, d_g, t_g = s_row[g], d_row[g], t_row[g]
        result = staged.at[side]
        for rows_at, here in project(result, g):
            y = result[rows_at, :] * s_g
            d_c, t_c, q_c = (columns[rows_at, c : c + 1] for c in (1, 2, 3))
            mixed = total[rows_at, pl.ds(pl.multiple_of(2 * side * wide, wide), wide)] * d_c
            square = total[rows_at, pl.ds(pl.multiple_of(2 * side * wide + wide, wide), wide)]
            off = jnp.where(here, t_c, mixed.astype(BF16).astype(F32))
            rounded = jnp.where(here, 0.0, square.astype(BF16).astype(F32))
            cube = q_c * off + t_g * rounded - y
            result[rows_at, :] = d_g * (
                jnp.where(here, 4.0, 0.0) - 6.0 * mixed + 4.0 * square - cube
            )

        @pl.when(side == 0)
        def _():
            far.start()

        @pl.when(side == 1)
        def _():
            near.start()

        return carry

    lax.fori_loop(0, 2 * nj, third_pass, 0)
    near, far = out_copies(stage, inv_out, inv_recv, 0)
    far.wait_send()
    near, far = out_copies(spare, inv_out, inv_recv, 0)
    near.wait()

    for j in range(nj):
        for landed, target in ((out_recv, e_out), (inv_recv, inv_out)):
            pltpu.make_async_remote_copy(
                src_ref=stage,
                dst_ref=target.at[j, pl.ds(pl.multiple_of((1 - k) * own, own), own), :],
                send_sem=send_sem.at[0],
                recv_sem=landed.at[j],
                device_id=sibling,
                device_id_type=MESH,
            ).wait_recv()

        for origin in range(cols):
            over(j, origin).wait_send()
            beside(0, j, origin).wait_send()
            beside(1, j, origin).wait_send()

            @pl.when((z < last) & (origin <= z))
            def _():
                up(j, origin).wait_send()

            @pl.when((z > 0) & (origin >= z))
            def _():
                down(j, origin).wait_send()


def in_one_kernel(pair_density, band_pairs, valence, conduction, wave_vectors, momentum, guess_scale):
    cols = lax.axis_size("col")
    rows = lax.axis_size("row")
    depth, height = pair_density.shape
    width = height * rows // cols
    wide = 2 * TILE
    nj = height // wide
    own = width // 2
    chunks = rows * nj
    pairs = depth * cols
    vm = pl.BlockSpec(memory_space=pltpu.VMEM)
    sm = pl.BlockSpec(memory_space=pltpu.SMEM)
    hbm = pl.BlockSpec(memory_space=pl.ANY)
    dma = pltpu.SemaphoreType.DMA
    body = functools.partial(gather_and_iterate, (depth, height, cols, wide, nj, own))
    e_turned, inverse_turned, _, _ = pl.pallas_call(
        body,
        out_shape=(
            jax.ShapeDtypeStruct((nj, width, wide), F32),
            jax.ShapeDtypeStruct((nj, width, wide), F32),
            jax.ShapeDtypeStruct((chunks, own, wide), F32),
            jax.ShapeDtypeStruct((2 * nj, own, wide), F32),
        ),
        in_specs=[hbm, vm, vm, sm, vm, sm, vm],
        out_specs=(hbm,) * 4,
        scratch_shapes=[
            pltpu.VMEM((chunks, pairs, wide), BF16),
            pltpu.VMEM((own, pairs), F32),
            pltpu.VMEM((own, pairs), BF16),
            pltpu.VMEM((2, own, wide), F32),
            pltpu.VMEM((own, wide), BF16),
            pltpu.VMEM((chunks, 1, wide), F32),
            pltpu.VMEM((chunks, 1, wide), F32),
            pltpu.VMEM((chunks, 1, wide), F32),
            pltpu.VMEM((1, pairs), F32),
            pltpu.VMEM((depth, 128), F32),
            pltpu.VMEM((own, 128), F32),
            dma((nj,)),
            dma((chunks, cols)),
            dma((nj, cols)),
            dma((nj, cols)),
            dma((nj, cols)),
            dma((2, nj, cols)),
            dma((nj,)),
            dma((nj,)),
            dma((6,)),
            dma((1,)),
        ],
        compiler_params=pltpu.CompilerParams(
            collective_id=0, has_side_effects=True, vmem_limit_bytes=67043328
        ),
    )(
        pair_density,
        band_pairs,
        valence.reshape(1, -1),
        conduction,
        wave_vectors,
        momentum,
        guess_scale.reshape(chunks, 1, wide),
    )

    def back(value):
        return jnp.swapaxes(value, 1, 2).reshape(height, width)

    return (back(e_turned), back(inverse_turned))


def solution(mesh):
    placed = (P(("pb", "col"), "row"), P(), P(), P(), P(None, "pb"), P("pb"), P("pb"))
    square_mesh = mesh.shape["row"] == 4 and mesh.shape["col"] == 4
    return jax.shard_map(
        in_one_kernel if square_mesh else on_device,
        mesh=mesh,
        in_specs=placed,
        out_specs=(P(("pb", "row"), "col"), P(("pb", "row"), "col")),
        check_vma=False,
    )
```
